128 devices in a mesh: dp: 16 (over x_hi, y, core), mp: 8 (over z, x_lo).
Axes of the slice: x: 4 (x_hi: 2, x_lo: 2; x = x_hi * 2 + x_lo), y: 4, z: 4, core: 2. Of those that a mesh axis runs over, the one named last changes fastest.
Arguments:
- target_states: bfloat16 [2048, 4096], P('dp', 'mp')
- target_gain: float32 [4096], replicated, may hold values from 0.1 to 1.9
- target_head: bfloat16 [4096, 128256], P(None, ('dp', 'mp'))
- reference_states: bfloat16 [2048, 2048], P(('dp', 'mp'))
- reference_gain: float32 [2048], replicated, may hold values from 0.1 to 1.9
- reference_head: bfloat16 [2048, 128256], P(None, ('dp', 'mp'))
- token_ids: int32 [2048], P('dp'), may hold values from 0 to 128255
- reference_order: int32 [16], replicated, may hold values from 0 to 15, each once
Outputs:
- target_loss: float32 [2048], P('dp')
- reference_loss: float32 [2048], P('dp')
- reducible: float32 [16], P('dp')
The draws below stay inside these ranges and needn't reach their ends.
Inputs may be any that keep to these rules, and one draw needn't show every extreme that they name: reference_states rows s * 128 to s * 128 + 127 belong to candidate sequence reference_order[s].
All inputs are finite; a program needn't handle non-finite values.
Results may differ from the reference program's by a relative error of at most 0.0041.
Values may be sent and summed in bfloat16 or wider, within the bound.
No kernel may reach another device: no remote copies, remote signals or barrier semaphores. Data moves between devices by JAX's collectives and lax.ppermute only.
A program may use at most 128 MiB of HBM per device.

```python
import math
import jax
import jax.numpy as jnp
import numpy as np
from jax import lax

D = 4096
DR = 2048
VOCAB = 128256
LENGTH = 128
SEQS = 16
TOKENS = 2048


def drawn_head(key, offset, breadth):
    raw_draw = jnp.clip(jax.random.normal(jax.random.fold_in(key, offset), (breadth, VOCAB), jnp.float32), -6.0, 6.0)
    column_ramp = 0.75 + 0.5 * jnp.arange(VOCAB, dtype=jnp.float32) / VOCAB
    return (raw_draw, column_ramp)


def entries_head(key, offset, breadth):
    raw_draw, column_ramp = drawn_head(key, offset, breadth)
    return raw_draw * (3.0 * column_ramp / math.sqrt(breadth))[None, :]


def drawn_states(key, offset, breadth):
    base_key = jax.random.fold_in(key, offset + 5)
    return jnp.clip(jax.random.normal(jax.random.fold_in(base_key, 1), (TOKENS, breadth), jnp.float32), -6.0, 6.0)


def draw_target_head(key, part):
    return entries_head(key, 10, D).astype(jnp.bfloat16)


def draw_reference_head(key, part):
    return entries_head(key, 20, DR).astype(jnp.bfloat16)


def draw_target_states(key, part):
    return drawn_states(key, 10, D).astype(jnp.bfloat16)


def draw_reference_states(key, part):
    return drawn_states(key, 20, DR).astype(jnp.bfloat16)


def with_ends(values, key, least, high):
    place = [jax.random.randint(jax.random.fold_in(key, axis), (), 0, length) for axis, length in enumerate(values.shape)]
    main_axis = values.shape.index(max(values.shape))
    next_to = place[:main_axis] + [(place[main_axis] + 1) % values.shape[main_axis]] + place[main_axis + 1:]
    return values.at[tuple(place)].set(least).at[tuple(next_to)].set(high)


def wide_ids(stream_key, shape, amount, lean):
    loads = [min(1 << octave, amount + 1 - (1 << octave)) * (1 << 20) // math.isqrt((1 << octave) ** lean) + 1 for octave in range((amount + 1).bit_length()) if 1 << octave <= amount]
    deviation = 1 + sum(loads) // (1 << 30)
    table = np.cumsum(np.array([max(1, weight // deviation) for weight in loads]))
    pick = jax.random.randint(jax.random.fold_in(stream_key, 1), shape, 0, int(table[len(loads) - 1]))
    start = jnp.left_shift(1, jnp.searchsorted(jnp.asarray(table, jnp.int32), pick, side="right").astype(jnp.int32))
    grade = start - 1 + jax.random.randint(jax.random.fold_in(stream_key, 4), shape, 0, 1 << 30) % jnp.minimum(start, amount + 1 - start)
    return jax.random.permutation(jax.random.fold_in(stream_key, 2), amount)[grade].astype(jnp.int32)


def setup_inputs(seed: int = 0) -> dict:
    seeds = jax.random.split(jax.random.key(seed), 9)
    return {
        "target_states": draw_target_states(jax.random.fold_in(seeds[8], 71), 0),
        "target_gain": jnp.clip(1.0 + 0.18 * jax.random.normal(seeds[1], (D,), jnp.float32), 0.1, 1.9),
        "target_head": draw_target_head(jax.random.fold_in(seeds[8], 71), 0),
        "reference_states": draw_reference_states(jax.random.fold_in(seeds[8], 71), 0),
        "reference_gain": jnp.clip(1.0 + 0.18 * jax.random.normal(seeds[4], (DR,), jnp.float32), 0.1, 1.9),
        "reference_head": draw_reference_head(jax.random.fold_in(seeds[8], 71), 0),
        "token_ids": with_ends(wide_ids(seeds[6], (TOKENS,), VOCAB, 2), jax.random.fold_in(seeds[6], 3), 0, VOCAB - 1).astype(jnp.int32),
        "reference_order": jax.random.permutation(seeds[7], SEQS).astype(jnp.int32),
    }


EPSILON = 1e-05

def normalize(states, gain):
    values = states.astype(jnp.float32)
    factor = lax.rsqrt(lax.optimization_barrier(jnp.mean(values * values, axis=1, keepdims=True)) + EPSILON)
    return (values * factor * gain.astype(jnp.float32)[None, :]).astype(jnp.bfloat16)

def losses(normed, head, ids):
    count = normed.shape[0]
    blocking = math.gcd(count, 256)

    def one_block(packed):
        rows_x, rows_id = packed
        logits = jnp.dot(rows_x, head, preferred_element_type=jnp.float32)
        peak_val = lax.optimization_barrier(jnp.max(logits, axis=1))
        log_total = peak_val + jnp.log(lax.optimization_barrier(jnp.sum(jnp.exp(logits - peak_val[:, None]), axis=1)))
        chosen = jnp.take_along_axis(logits, rows_id[:, None], axis=1)[:, 0]
        return log_total - chosen
    stacked = lax.map(one_block, (normed.reshape(-1, blocking, normed.shape[1]), ids.reshape(-1, blocking)))
    return stacked.reshape(count)

def reference(target_states, target_gain, target_head, reference_states, reference_gain, reference_head, token_ids, reference_order):
    target_loss = losses(normalize(target_states, target_gain), target_head, token_ids)
    seq_ids = token_ids.reshape(SEQS, LENGTH)
    reference_ids = jnp.take(seq_ids, reference_order.astype(jnp.int32), axis=0).reshape(TOKENS)
    rows_loss = losses(normalize(reference_states, reference_gain), reference_head, reference_ids)
    matches = (reference_order[:, None] == jnp.arange(SEQS, dtype=jnp.int32)[None, :]).astype(jnp.float32)
    reference_loss = lax.optimization_barrier(jnp.sum(matches[:, :, None] * rows_loss.reshape(SEQS, LENGTH)[:, None, :], axis=0)).reshape(TOKENS)
    reducible = lax.optimization_barrier(jnp.mean((target_loss - reference_loss).reshape(SEQS, LENGTH), axis=1))
    return (target_loss, reference_loss, reducible)
```

```python
import functools

import jax
import jax.numpy as jnp
from jax import lax
from jax.experimental import pallas as pl
from jax.experimental.pallas import tpu as pltpu
from jax.sharding import Mesh
from jax.sharding import PartitionSpec as P


LENGTH = 128
SEQS = 16
EPSILON = 1e-05
LANES = 128
TILE = 256
AXES = ("xh", "y", "c", "z", "xl")
CHIPS = ("xh", "y", "z", "xl")
DP = ("xh", "y", "c")
MP = ("z", "xl")


def linear(x, y, z, c):
    return ((((x // 2) * 4 + y) * 2 + c) * 4 + z) * 2 + x % 2


def route(move):
    pairs = []
    for x in range(4):
        for y in range(4):
            for z in range(4):
                for c in range(2):
                    pairs.append((linear(x, y, z, c), linear(*move(x, y, z, c))))
    return pairs


def sent(values, move):
    return lax.ppermute(values, AXES, route(move))


def sibling(x, y, z, c):
    return x, y, z, 1 - c


def mask_of(step, core):
    return 1 if step == core else 3


def paired(axis, step):
    def move(x, y, z, c):
        at = {"x": x, "y": y, "z": z}
        at[axis] ^= mask_of(step, c)
        return at["x"], at["y"], at["z"], c

    return move


def normalize(states, gain):
    values = states.astype(jnp.float32)
    factor = lax.rsqrt(jnp.mean(values * values, axis=1, keepdims=True) + EPSILON)
    return (values * factor * gain[None, :]).astype(jnp.bfloat16)


def here():
    return {
        "x": lax.axis_index("xh") * 2 + lax.axis_index("xl"),
        "y": lax.axis_index("y"),
        "z": lax.axis_index("z"),
        "c": lax.axis_index("c"),
    }


def chip_of_block(block, order, me):
    at = {a: me[a] for a in "xyz"}
    for phase, axis in enumerate(order):
        for step in range(2):
            mask = jnp.where(me["c"] == step, 1, 3)
            at[axis] = at[axis] ^ jnp.where((block >> (2 * phase + step)) & 1 == 1, mask, 0)
    return at


def row_place(order, rows, offset, top, me):
    k = jnp.arange(16 * rows, dtype=jnp.int32)
    at = chip_of_block(k // rows + 16 * top, order, me)
    sequence = ((at["x"] >> 1) * 4 + at["y"]) * 2 + me["c"]
    return sequence, (at["z"] * 2 + (at["x"] & 1)) * 16 + offset + k % rows


def loss_kernel(count, width, base_ref, *refs):
    pieces, (ids_ref, own_ref, sib_ref, out_ref, rows_ref, top_ref, sum_ref, hit_ref) = (
        refs[:count],
        refs[count:],
    )
    j = pl.program_id(0)

    @pl.when(j == 0)
    def _():
        at = 0
        for piece in pieces:
            rows_ref[at : at + piece.shape[0], :] = piece[...]
            at += piece.shape[0]
        top_ref[...] = jnp.full_like(top_ref, -jnp.inf)
        sum_ref[...] = jnp.zeros_like(sum_ref)
        hit_ref[...] = jnp.zeros_like(hit_ref)

    x = rows_ref[...]
    first = j * TILE
    lane = lax.broadcasted_iota(jnp.int32, (x.shape[0], LANES), 1)
    groups = []
    ids = ids_ref[...]
    hit = hit_ref[...]
    top = top_ref[...]
    best = top
    for side, head_ref in enumerate((own_ref, sib_ref)):
        logits = jnp.dot(x, head_ref[...], preferred_element_type=jnp.float32)
        for g in range(TILE // LANES):
            column = lane + (first + g * LANES)
            part = jnp.where(column < width, logits[:, g * LANES : (g + 1) * LANES], -jnp.inf)
            wanted = jnp.where(column < width, column + base_ref[side], -1) == ids
            hit = hit + jnp.where(wanted, part, 0.0)
            best = jnp.maximum(best, part)
            groups.append(part)
    total = sum_ref[...] * jnp.exp(top - best)
    for part in groups:
        total = total + jnp.exp(part - best)
    top_ref[...] = best
    sum_ref[...] = total
    hit_ref[...] = hit

    @pl.when(j == pl.num_programs(0) - 1)
    def _():
        for r in range(0, x.shape[0], LANES):
            tops = top_ref[r : r + LANES, :].T
            sums = sum_ref[r : r + LANES, :].T
            hits = hit_ref[r : r + LANES, :].T
            peak = jnp.max(tops, axis=0, keepdims=True)
            whole = jnp.sum(sums * jnp.exp(tops - peak), axis=0, keepdims=True)
            out_ref[0:1, r : r + LANES] = peak + jnp.log(whole)
            out_ref[1:2, r : r + LANES] = jnp.sum(hits, axis=0, keepdims=True)


def losses(pieces, ids, own, other, bases):
    rows = sum(p.shape[0] for p in pieces)
    depth, width = own.shape
    whole = lambda shape: pl.BlockSpec(shape, lambda j: (0, 0))
    tile = pl.BlockSpec((depth, TILE), lambda j: (0, j))
    steps = pl.cdiv(width, TILE)
    return pl.pallas_call(
        functools.partial(loss_kernel, len(pieces), width),
        grid=(steps,),
        in_specs=[pl.BlockSpec(memory_space=pltpu.SMEM)]
        + [whole(p.shape) for p in pieces]
        + [whole((rows, LANES)), tile, tile],
        out_specs=whole((2, rows)),
        out_shape=jax.ShapeDtypeStruct((2, rows), jnp.float32),
        scratch_shapes=[
            pltpu.VMEM((rows, depth), jnp.bfloat16),
            pltpu.VMEM((rows, LANES), jnp.float32),
            pltpu.VMEM((rows, LANES), jnp.float32),
            pltpu.VMEM((rows, LANES), jnp.float32),
        ],
        cost_estimate=pl.CostEstimate(
            flops=4 * rows * depth * width,
            bytes_accessed=4 * depth * width + 2 * rows * depth,
            transcendentals=2 * rows * width,
        ),
        name=f"losses_{depth}_{rows}",
    )(bases, *pieces, ids, own, other)


def split_dot(values, places):
    high = lax.reduce_precision(values, 8, 7)
    middle = lax.reduce_precision(values - high, 8, 7)
    low = (values - high) - middle
    parts = jnp.dot(
        jnp.concatenate([high, middle, low]).astype(jnp.bfloat16), places, preferred_element_type=jnp.float32
    )
    k = values.shape[0]
    return (parts[:k] + parts[k : 2 * k]) + parts[2 * k :]


ORDERS = {"r": "xyz", "a": "zxy", "b": "yzx"}


def shards(
    target_states,
    target_gain,
    target_head,
    reference_states,
    reference_gain,
    reference_head,
    token_ids,
    reference_order,
):
    me = here()
    width = target_head.shape[1]
    my_place = lax.axis_index(AXES)
    bases = jnp.stack([my_place, my_place ^ 8]).astype(jnp.int32) * width

    blocks = {"r": normalize(reference_states, reference_gain)}
    mine = lax.all_to_all(target_states.reshape(8, 16, 512), MP, 0, 0, tiled=True)
    mine = normalize(jnp.moveaxis(mine, 0, 1).reshape(16, 4096), target_gain)
    blocks["a"], blocks["b"] = mine[:8], mine[8:]

    other_target = sent(target_head, sibling)
    other_reference = sent(reference_head, sibling)

    for phase in range(2):
        for step in range(2):
            for k in "rab":
                got = sent(blocks[k], paired(ORDERS[k][phase], step))
                blocks[k] = jnp.concatenate([blocks[k], got])
    quarters = {}
    for k in "rab":
        axis = ORDERS[k][2]
        quarters[k] = [blocks[k], sent(blocks[k], paired(axis, 0)), sent(blocks[k], paired(axis, 1))]
    for k in "rab":
        quarters[k].append(sent(quarters[k][1], paired(ORDERS[k][2], 1)))

    table = token_ids.reshape(1, LENGTH)
    moves = [
        lambda x, y, z, c: (x, y, z, 1 - c),
        lambda x, y, z, c: (x, y ^ 1, z, c),
        lambda x, y, z, c: (x, y ^ 3, z, c),
        lambda x, y, z, c: (x ^ 3, y, z, c),
    ]
    for move in moves:
        table = jnp.concatenate([table, sent(table, move)])
    k = jnp.arange(SEQS, dtype=jnp.int32)
    table_y = me["y"] ^ ((k >> 1) & 1) ^ (((k >> 2) & 1) * 3)
    table_x = (me["x"] >> 1) ^ ((k >> 3) & 1)
    table_seq = (table_x * 4 + table_y) * 2 + (me["c"] ^ (k & 1))
    table_token = (table_seq[:, None] * LENGTH + jnp.arange(LENGTH, dtype=jnp.int32)).reshape(-1)
    table = table.reshape(-1)

    def looked_up(tokens):
        found = jnp.where(tokens[:, None] == table_token[None, :], table[None, :], 0)
        return jnp.broadcast_to(jnp.sum(found, axis=1, keepdims=True), (tokens.shape[0], LANES))

    def candidate_of(sequence):
        same = sequence[:, None] == jnp.arange(SEQS, dtype=jnp.int32)[None, :]
        return jnp.sum(jnp.where(same, reference_order[None, :], 0), axis=1)

    passes = ((0,), (1, 2), (3,))
    bits = {0: 0, 1: 1, 2: 2, 3: 3}
    target_stats, reference_stats, target_at, reference_at = [], [], [], []
    for group in passes:
        places = [row_place(ORDERS["r"], 16, 0, bits[q], me) for q in group]
        at = jnp.concatenate([candidate_of(s) * LENGTH + p for s, p in places])
        reference_at.append(at)
        reference_stats.append(
            losses(
                [quarters["r"][q] for q in group],
                looked_up(at),
                reference_head,
                other_reference,
                bases,
            )
        )
        places = [
            row_place(ORDERS[m], 8, 8 * (m == "b"), bits[q], me) for q in group for m in "ab"
        ]
        at = jnp.concatenate([s * LENGTH + p for s, p in places])
        target_at.append(jnp.concatenate([(s >> 1) * LENGTH + p for s, p in places]))
        target_stats.append(
            losses(
                [quarters[m][q] for q in group for m in "ab"],
                looked_up(at),
                target_head,
                other_target,
                bases,
            )
        )

    def put(stats, at, size):
        where = jnp.concatenate(at)
        places = (where[:, None] == jnp.arange(size, dtype=jnp.int32)[None, :]).astype(jnp.bfloat16)
        return split_dot(jnp.concatenate(stats, axis=1), places)

    tokens = SEQS * LENGTH
    target_put = put(target_stats, target_at, tokens // 2).reshape(2, 8, 1, LENGTH)
    reference_put = put(reference_stats, reference_at, tokens).reshape(2, 8, 2, LENGTH)
    payload = jnp.concatenate([target_put, reference_put], axis=2)
    payload = jnp.moveaxis(payload, 0, 1).reshape(8, 1, 6, LENGTH)
    payload = jnp.pad(payload, ((0, 0), (0, 0), (0, 2), (0, 0)))
    payload = jnp.broadcast_to(payload, (8, 8, 8, LENGTH)).reshape(64, 8, LENGTH)
    parts = lax.all_to_all(payload, CHIPS, 0, 0, tiled=True)
    peak = jnp.max(parts[:, :3], axis=0)
    whole = peak + jnp.log(jnp.sum(jnp.exp(parts[:, :3] - peak[None]), axis=0))
    loss = whole - jnp.sum(parts[:, 3:6], axis=0)

    core = me["c"]
    mine_target = loss[0]
    kept = jnp.where(core == 0, loss[1], loss[2])
    given = jnp.where(core == 0, loss[2], loss[1])
    taken = sent(given[None], sibling)[0]
    candidate = lax.axis_index(DP)
    holder = jnp.sum(jnp.where(reference_order == candidate, k & 1, 0))
    mine_reference = jnp.where(holder == core, kept, taken)
    reducible = jnp.mean(mine_target - mine_reference).reshape(1)
    return mine_target, mine_reference, reducible


def solution(mesh):
    torus = Mesh(mesh.devices.reshape(2, 4, 2, 4, 2), AXES)
    in_specs = (P(DP, MP), P(), P(None, AXES), P(AXES, None), P(), P(None, AXES), P(DP), P())
    out_specs = (P(DP), P(DP), P(DP))
    return jax.shard_map(
        shards, mesh=torus, in_specs=in_specs, out_specs=out_specs, check_vma=False
    )
```

```python
import functools

import jax
import jax.numpy as jnp
from jax import lax
from jax.experimental import pallas as pl
from jax.experimental.pallas import tpu as pltpu
from jax.sharding import Mesh
from jax.sharding import PartitionSpec as P


LENGTH = 128
SEQS = 16
EPSILON = 1e-05
LANES = 128
TILE = 256
AXES = ("xh", "y", "c", "z", "xl")
CHIPS = ("xh", "y", "z", "xl")
DP = ("xh", "y", "c")
MP = ("z", "xl")


def linear(x, y, z, c):
    return ((((x // 2) * 4 + y) * 2 + c) * 4 + z) * 2 + x % 2


def route(move):
    pairs = []
    for x in range(4):
        for y in range(4):
            for z in range(4):
                for c in range(2):
                    pairs.append((linear(x, y, z, c), linear(*move(x, y, z, c))))
    return pairs


def sent(values, move):
    return lax.ppermute(values, AXES, route(move))


def sibling(x, y, z, c):
    return x, y, z, 1 - c


def paired(axes, masks):
    def move(x, y, z, c):
        at = {"x": x, "y": y, "z": z}
        at[axes[c]] ^= masks[c]
        return at["x"], at["y"], at["z"], c

    return move


def normalize(states, gain):
    values = states.astype(jnp.float32)
    factor = lax.rsqrt(jnp.mean(values * values, axis=1, keepdims=True) + EPSILON)
    return (values * factor * gain[None, :]).astype(jnp.bfloat16)


def here():
    return {
        "x": lax.axis_index("xh") * 2 + lax.axis_index("xl"),
        "y": lax.axis_index("y"),
        "z": lax.axis_index("z"),
        "c": lax.axis_index("c"),
    }


def chip_of_block(block, phases, me):
    at = {a: me[a] for a in "xyz"}
    for phase, steps in enumerate(phases):
        for step, (axes, masks) in enumerate(steps):
            came = (block >> (2 * phase + step)) & 1
            for core in range(2):
                moved = jnp.where(me["c"] == core, came * masks[core], 0)
                at[axes[core]] = at[axes[core]] ^ moved
    return at


def row_place(phases, blocks, me):
    k = jnp.arange(16 * len(blocks), dtype=jnp.int32)
    block = jnp.concatenate([jnp.full((16,), b, jnp.int32) for b in blocks])
    at = chip_of_block(block, phases, me)
    sequence = ((at["x"] >> 1) * 4 + at["y"]) * 2 + me["c"]
    return sequence, (at["z"] * 2 + (at["x"] & 1)) * 16 + k % 16


def loss_kernel(count, width, base_ref, *refs):
    pieces, (ids_ref, own_ref, sib_ref, out_ref, rows_ref, top_ref, sum_ref, hit_ref) = (
        refs[:count],
        refs[count:],
    )
    j = pl.program_id(0)

    @pl.when(j == 0)
    def _():
        at = 0
        for piece in pieces:
            rows_ref[at : at + piece.shape[0], :] = piece[...]
            at += piece.shape[0]
        top_ref[...] = jnp.full_like(top_ref, -jnp.inf)
        sum_ref[...] = jnp.zeros_like(sum_ref)
        hit_ref[...] = jnp.zeros_like(hit_ref)

    x = rows_ref[...]
    first = j * TILE
    lane = lax.broadcasted_iota(jnp.int32, (x.shape[0], LANES), 1)
    groups = []
    ids = ids_ref[...]
    hit = hit_ref[...]
    top = top_ref[...]
    best = top
    for side, head_ref in enumerate((own_ref, sib_ref)):
        logits = lax.dot_general(
            x, head_ref[...], (((1,), (1,)), ((), ())), preferred_element_type=jnp.float32
        )
        for g in range(TILE // LANES):
            column = lane + (first + g * LANES)
            part = jnp.where(column < width, logits[:, g * LANES : (g + 1) * LANES], -jnp.inf)
            wanted = jnp.where(column < width, column + base_ref[side], -1) == ids
            hit = hit + jnp.where(wanted, part, 0.0)
            best = jnp.maximum(best, part)
            groups.append(part)
    total = sum_ref[...] * jnp.exp(top - best)
    for part in groups:
        total = total + jnp.exp(part - best)
    top_ref[...] = best
    sum_ref[...] = total
    hit_ref[...] = hit

    @pl.when(j == pl.num_programs(0) - 1)
    def _():
        for r in range(0, x.shape[0], LANES):
            tops = top_ref[r : r + LANES, :].T
            sums = sum_ref[r : r + LANES, :].T
            hits = hit_ref[r : r + LANES, :].T
            peak = jnp.max(tops, axis=0, keepdims=True)
            whole = jnp.sum(sums * jnp.exp(tops - peak), axis=0, keepdims=True)
            out_ref[0:1, r : r + LANES] = peak + jnp.log(whole)
            out_ref[1:2, r : r + LANES] = jnp.sum(hits, axis=0, keepdims=True)


def losses(pieces, ids, part, own, other, bases):
    rows = sum(p.shape[0] for p in pieces)
    width, depth = own.shape
    whole = lambda shape: pl.BlockSpec(shape, lambda j: (0, 0))
    tile = pl.BlockSpec((TILE, depth), lambda j: (j, 0))
    steps = pl.cdiv(width, TILE)
    return pl.pallas_call(
        functools.partial(loss_kernel, len(pieces), width),
        grid=(steps,),
        in_specs=[pl.BlockSpec(memory_space=pltpu.SMEM)]
        + [whole(p.shape) for p in pieces]
        + [pl.BlockSpec((rows, LANES), lambda j: (part, 0)), tile, tile],
        out_specs=whole((2, rows)),
        out_shape=jax.ShapeDtypeStruct((2, rows), jnp.float32),
        scratch_shapes=[
            pltpu.VMEM((rows, depth), jnp.bfloat16),
            pltpu.VMEM((rows, LANES), jnp.float32),
            pltpu.VMEM((rows, LANES), jnp.float32),
            pltpu.VMEM((rows, LANES), jnp.float32),
        ],
        cost_estimate=pl.CostEstimate(
            flops=4 * rows * depth * width,
            bytes_accessed=4 * depth * width + 2 * rows * depth,
            transcendentals=2 * rows * width,
        ),
        name=f"losses_{depth}_{rows}",
    )(bases, *pieces, ids, own, other)


def split_dot(values, places):
    high = lax.reduce_precision(values, 8, 7)
    middle = lax.reduce_precision(values - high, 8, 7)
    low = (values - high) - middle
    parts = jnp.dot(
        jnp.concatenate([high, middle, low]).astype(jnp.bfloat16), places, preferred_element_type=jnp.float32
    )
    k = values.shape[0]
    return (parts[:k] + parts[k : 2 * k]) + parts[2 * k :]


REFERENCE = [[((a, a), (1, 3)), ((a, a), (3, 1))] for a in "yzx"]
TARGET = [[(a, (1, 1)), (a, (3, 3))] for a in ("xz", "yx", "zy")]


def shards(
    target_states,
    target_gain,
    target_head,
    reference_states,
    reference_gain,
    reference_head,
    token_ids,
    reference_order,
):
    me = here()
    width = target_head.shape[1]
    my_place = lax.axis_index(AXES)
    bases = jnp.stack([my_place, my_place ^ 8]).astype(jnp.int32) * width

    mine = lax.all_to_all(target_states.reshape(8, 16, 512), MP, 0, 0, tiled=True)
    r = normalize(reference_states, reference_gain)
    own_target, own_reference = target_head.T, reference_head.T
    r = jnp.concatenate([r, sent(r, paired(*REFERENCE[0][0]))])
    r = jnp.concatenate([r, sent(r, paired(*REFERENCE[0][1]))])
    other_reference = sent(own_reference, sibling)
    other_target = sent(own_target, sibling)
    t = normalize(jnp.moveaxis(mine, 0, 1).reshape(16, 4096), target_gain)
    t = jnp.concatenate([t, sent(t, paired(*TARGET[0][0]))])
    r = jnp.concatenate([r, sent(r, paired(*REFERENCE[1][0]))])
    t = jnp.concatenate([t, sent(t, paired(*TARGET[0][1]))])
    r = jnp.concatenate([r, sent(r, paired(*REFERENCE[1][1]))])

    first, second = (paired(*step) for step in TARGET[1])
    t_first, t_second = sent(t, first), sent(t, second)
    low = jnp.concatenate([t, t_first])
    r_first = sent(r, paired(*REFERENCE[2][0]))
    r_second = sent(r, paired(*REFERENCE[2][1]))
    high = jnp.concatenate([t_second, sent(t_first, second)])

    first, second = (paired(*step) for step in TARGET[2])
    low_first, high_second = sent(low, first), sent(high, second)
    high_first, low_second = sent(high, first), sent(low, second)
    r_both = sent(r_first, paired(*REFERENCE[2][1]))
    low_both, high_both = sent(low_first, second), sent(high_second, first)
    target_passes = (
        (low, high, low_first, high_second),
        (high_first, low_second, low_both, high_both),
    )
    target_blocks = [*range(24), *range(40, 48), *range(24, 40), *range(48, 64)]

    table = token_ids.reshape(1, LENGTH)
    moves = [
        lambda x, y, z, c: (x, y, z, 1 - c),
        lambda x, y, z, c: (x, y ^ 1, z, c),
        lambda x, y, z, c: (x, y ^ 3, z, c),
        lambda x, y, z, c: (x ^ 3, y, z, c),
    ]
    for move in moves:
        table = jnp.concatenate([table, sent(table, move)])
    k = jnp.arange(SEQS, dtype=jnp.int32)
    table_y = me["y"] ^ ((k >> 1) & 1) ^ (((k >> 2) & 1) * 3)
    table_x = (me["x"] >> 1) ^ ((k >> 3) & 1)
    table_seq = (table_x * 4 + table_y) * 2 + (me["c"] ^ (k & 1))
    table_token = (table_seq[:, None] * LENGTH + jnp.arange(LENGTH, dtype=jnp.int32)).reshape(-1)
    table = table.reshape(-1)

    def looked_up(tokens):
        found = jnp.where(tokens[:, None] == table_token[None, :], table[None, :], 0)
        return jnp.broadcast_to(jnp.sum(found, axis=1, keepdims=True), (tokens.shape[0], LANES))

    def candidate_of(sequence):
        same = sequence[:, None] == jnp.arange(SEQS, dtype=jnp.int32)[None, :]
        return jnp.sum(jnp.where(same, reference_order[None, :], 0), axis=1)

    sequence, position = row_place(REFERENCE, range(64), me)
    reference_at = candidate_of(sequence) * LENGTH + position
    reference_ids = looked_up(reference_at)
    sequence, position = row_place(TARGET, target_blocks, me)
    target_at = (sequence >> 1) * LENGTH + position
    target_ids = looked_up(sequence * LENGTH + position)

    target_stats = [
        losses(target_passes[0], target_ids, 0, own_target, other_target, bases)
    ]
    reference_bases, target_stats[0] = lax.optimization_barrier((bases, target_stats[0]))
    reference_stats = [
        losses(
            (r, r_first, r_second, r_both),
            reference_ids,
            0,
            own_reference,
            other_reference,
            reference_bases,
        )
    ]
    target_stats.append(
        losses(target_passes[1], target_ids, 1, own_target, other_target, bases)
    )

    def put(stats, at, size):
        places = (at[:, None] == jnp.arange(size, dtype=jnp.int32)[None, :]).astype(jnp.bfloat16)
        return split_dot(jnp.concatenate(stats, axis=1), places)

    tokens = SEQS * LENGTH
    target_put = put(target_stats, target_at, tokens // 2).reshape(2, 8, 1, LENGTH)
    reference_put = put(reference_stats, reference_at, tokens).reshape(2, 8, 2, LENGTH)
    payload = jnp.concatenate([target_put, reference_put], axis=2)
    payload = jnp.moveaxis(payload, 0, 1).reshape(8, 1, 6, LENGTH)
    payload = jnp.pad(payload, ((0, 0), (0, 0), (0, 2), (0, 0)))
    payload = jnp.broadcast_to(payload, (8, 8, 8, LENGTH)).reshape(64, 8, LENGTH)
    parts = lax.all_to_all(payload, CHIPS, 0, 0, tiled=True)
    peak = jnp.max(parts[:, :3], axis=0)
    whole = peak + jnp.log(jnp.sum(jnp.exp(parts[:, :3] - peak[None]), axis=0))
    loss = whole - jnp.sum(parts[:, 3:6], axis=0)

    core = me["c"]
    mine_target = loss[0]
    kept = jnp.where(core == 0, loss[1], loss[2])
    given = jnp.where(core == 0, loss[2], loss[1])
    taken = sent(given[None], sibling)[0]
    candidate = lax.axis_index(DP)
    holder = jnp.sum(jnp.where(reference_order == candidate, k & 1, 0))
    mine_reference = jnp.where(holder == core, kept, taken)
    reducible = jnp.mean(mine_target - mine_reference).reshape(1)
    return mine_target, mine_reference, reducible


def solution(mesh):
    torus = Mesh(mesh.devices.reshape(2, 4, 2, 4, 2), AXES)
    in_specs = (P(DP, MP), P(), P(None, AXES), P(AXES, None), P(), P(None, AXES), P(DP), P())
    out_specs = (P(DP), P(DP), P(DP))
    return jax.shard_map(
        shards, mesh=torus, in_specs=in_specs, out_specs=out_specs, check_vma=False
    )
```

```python
import functools

import jax
import jax.numpy as jnp
from jax import lax
from jax.experimental import pallas as pl
from jax.experimental.pallas import tpu as pltpu
from jax.sharding import Mesh
from jax.sharding import PartitionSpec as P


LENGTH = 128
SEQS = 16
EPSILON = 1e-05
LANES = 128
TILE = 256
AXES = ("xh", "y", "c", "z", "xl")
CHIPS = ("xh", "y", "z", "xl")
DP = ("xh", "y", "c")
MP = ("z", "xl")


def linear(x, y, z, c):
    return ((((x // 2) * 4 + y) * 2 + c) * 4 + z) * 2 + x % 2


def route(move):
    pairs = []
    for x in range(4):
        for y in range(4):
            for z in range(4):
                for c in range(2):
                    pairs.append((linear(x, y, z, c), linear(*move(x, y, z, c))))
    return pairs


def sent(values, move):
    return lax.ppermute(values, AXES, route(move))


def sibling(x, y, z, c):
    return x, y, z, 1 - c


def paired(axes, masks):
    def move(x, y, z, c):
        at = {"x": x, "y": y, "z": z}
        at[axes[c]] ^= masks[c]
        return at["x"], at["y"], at["z"], c

    return move


def after(values, others):
    return lax.optimization_barrier((values, others))[0]


def normalize(states, gain):
    values = states.astype(jnp.float32)
    factor = lax.rsqrt(jnp.mean(values * values, axis=1, keepdims=True) + EPSILON)
    return (values * factor * gain[None, :]).astype(jnp.bfloat16)


def here():
    return {
        "x": lax.axis_index("xh") * 2 + lax.axis_index("xl"),
        "y": lax.axis_index("y"),
        "z": lax.axis_index("z"),
        "c": lax.axis_index("c"),
    }


def chip_of_block(block, phases, me):
    at = {a: me[a] for a in "xyz"}
    for phase, steps in enumerate(phases):
        for step, (axes, masks) in enumerate(steps):
            came = (block >> (2 * phase + step)) & 1
            for core in range(2):
                moved = jnp.where(me["c"] == core, came * masks[core], 0)
                at[axes[core]] = at[axes[core]] ^ moved
    return at


def row_place(phases, blocks, me):
    k = jnp.arange(16 * len(blocks), dtype=jnp.int32)
    block = jnp.concatenate([jnp.full((16,), b, jnp.int32) for b in blocks])
    at = chip_of_block(block, phases, me)
    sequence = ((at["x"] >> 1) * 4 + at["y"]) * 2 + me["c"]
    return sequence, (at["z"] * 2 + (at["x"] & 1)) * 16 + k % 16


def loss_kernel(count, width, base_ref, *refs):
    pieces, (ids_ref, own_ref, sib_ref, out_ref, rows_ref, top_ref, sum_ref, hit_ref) = (
        refs[:count],
        refs[count:],
    )
    j = pl.program_id(0)

    @pl.when(j == 0)
    def _():
        at = 0
        for piece in pieces:
            rows_ref[at : at + piece.shape[0], :] = piece[...]
            at += piece.shape[0]
        top_ref[...] = jnp.full_like(top_ref, -jnp.inf)
        sum_ref[...] = jnp.zeros_like(sum_ref)
        hit_ref[...] = jnp.zeros_like(hit_ref)

    x = rows_ref[...]
    size = own_ref.shape[0]
    first = j * size
    lane = lax.broadcasted_iota(jnp.int32, (x.shape[0], LANES), 1)
    groups = []
    ids = ids_ref[...]
    hit = hit_ref[...]
    top = top_ref[...]
    best = top
    for side, head_ref in enumerate((own_ref, sib_ref)):
        logits = lax.dot_general(
            x, head_ref[...], (((1,), (1,)), ((), ())), preferred_element_type=jnp.float32
        )
        for g in range(size // LANES):
            column = lane + (first + g * LANES)
            part = jnp.where(column < width, logits[:, g * LANES : (g + 1) * LANES], -jnp.inf)
            wanted = jnp.where(column < width, column + base_ref[side], -1) == ids
            hit = hit + jnp.where(wanted, part, 0.0)
            best = jnp.maximum(best, part)
            groups.append(part)
    total = sum_ref[...] * jnp.exp(top - best)
    for part in groups:
        total = total + jnp.exp(part - best)
    top_ref[...] = best
    sum_ref[...] = total
    hit_ref[...] = hit

    @pl.when(j == pl.num_programs(0) - 1)
    def _():
        for r in range(0, x.shape[0], LANES):
            tops = top_ref[r : r + LANES, :].T
            sums = sum_ref[r : r + LANES, :].T
            hits = hit_ref[r : r + LANES, :].T
            peak = jnp.max(tops, axis=0, keepdims=True)
            whole = jnp.sum(sums * jnp.exp(tops - peak), axis=0, keepdims=True)
            out_ref[0:1, r : r + LANES] = peak + jnp.log(whole)
            out_ref[1:2, r : r + LANES] = jnp.sum(hits, axis=0, keepdims=True)


def losses(pieces, ids, own, other, bases):
    rows = sum(p.shape[0] for p in pieces)
    width, depth = own.shape
    whole = lambda shape: pl.BlockSpec(shape, lambda j: (0, 0))
    size = 2 * TILE if depth <= 2048 else TILE
    tile = pl.BlockSpec((size, depth), lambda j: (j, 0))
    steps = pl.cdiv(width, size)
    return pl.pallas_call(
        functools.partial(loss_kernel, len(pieces), width),
        grid=(steps,),
        in_specs=[pl.BlockSpec(memory_space=pltpu.SMEM)]
        + [whole(p.shape) for p in pieces]
        + [whole((rows, LANES)), tile, tile],
        out_specs=whole((2, rows)),
        out_shape=jax.ShapeDtypeStruct((2, rows), jnp.float32),
        scratch_shapes=[
            pltpu.VMEM((rows, depth), jnp.bfloat16),
            pltpu.VMEM((rows, LANES), jnp.float32),
            pltpu.VMEM((rows, LANES), jnp.float32),
            pltpu.VMEM((rows, LANES), jnp.float32),
        ],
        cost_estimate=pl.CostEstimate(
            flops=4 * rows * depth * width,
            bytes_accessed=4 * depth * width + 2 * rows * depth,
            transcendentals=2 * rows * width,
        ),
        name=f"losses_{depth}_{rows}",
    )(bases, *pieces, ids, own, other)


def split_dot(values, places):
    high = lax.reduce_precision(values, 8, 7)
    middle = lax.reduce_precision(values - high, 8, 7)
    low = (values - high) - middle
    parts = jnp.dot(
        jnp.concatenate([high, middle, low]).astype(jnp.bfloat16), places, preferred_element_type=jnp.float32
    )
    k = values.shape[0]
    return (parts[:k] + parts[k : 2 * k]) + parts[2 * k :]


REFERENCE = [[((a, a), (1, 3)), ((a, a), (3, 1))] for a in "yzx"]
TARGET = [[(a, (1, 1)), (a, (3, 3))] for a in ("xz", "yx", "zy")]


def shards(
    target_states,
    target_gain,
    target_head,
    reference_states,
    reference_gain,
    reference_head,
    token_ids,
    reference_order,
):
    me = here()
    width = target_head.shape[1]
    my_place = lax.axis_index(AXES)
    bases = jnp.stack([my_place, my_place ^ 8]).astype(jnp.int32) * width

    own_target, own_reference = target_head.T, reference_head.T
    mine = lax.all_to_all(target_states.reshape(8, 16, 512), MP, 0, 0, tiled=True)
    ids = [token_ids.reshape(1, LENGTH)]
    ids.append(sent(ids[0], sibling))
    t = normalize(jnp.moveaxis(mine, 0, 1).reshape(16, 4096), target_gain)
    t = after(t, ids[-1])
    r = normalize(reference_states, reference_gain)
    other_target = sent(own_target, sibling)
    other_reference = sent(own_reference, sibling)

    def more_ids(move):
        ids.append(sent(jnp.concatenate(ids), move))

    t = jnp.concatenate([t, sent(t, paired(*TARGET[0][0]))])
    more_ids(lambda x, y, z, c: (x, y ^ 1, z, c))
    r = jnp.concatenate([r, sent(r, paired(*REFERENCE[0][0]))])
    t = after(t, ids[-1])
    t = jnp.concatenate([t, sent(t, paired(*TARGET[0][1]))])
    more_ids(lambda x, y, z, c: (x, y ^ 3, z, c))
    r = jnp.concatenate([r, sent(r, paired(*REFERENCE[0][1]))])
    t = after(t, ids[-1])
    more_ids(lambda x, y, z, c: (x ^ 3, y, z, c))
    r = jnp.concatenate([r, sent(r, paired(*REFERENCE[1][0]))])
    r = jnp.concatenate([r, sent(r, paired(*REFERENCE[1][1]))])

    first, second = (paired(*step) for step in TARGET[1])
    t_first, t_second = sent(t, first), sent(t, second)
    low = jnp.concatenate([t, t_first])
    r_first = sent(r, paired(*REFERENCE[2][0]))
    r_second = sent(r, paired(*REFERENCE[2][1]))
    high = jnp.concatenate([t_second, sent(after(t_first, ids[-1]), second)])

    first, second = (paired(*step) for step in TARGET[2])
    low_first, high_second = sent(low, first), sent(high, second)
    high_first, low_second = sent(high, first), sent(low, second)
    r_both = sent(r_first, paired(*REFERENCE[2][1]))
    low_both, high_both = sent(low_first, second), sent(high_second, first)
    target_passes = (
        (low, high, low_first, high_second),
        (high_first, low_second, low_both, high_both),
    )
    target_blocks = [*range(24), *range(40, 48), *range(24, 40), *range(48, 64)]

    table = jnp.concatenate(ids)
    k = jnp.arange(SEQS, dtype=jnp.int32)
    table_y = me["y"] ^ ((k >> 1) & 1) ^ (((k >> 2) & 1) * 3)
    table_x = (me["x"] >> 1) ^ ((k >> 3) & 1)
    table_seq = (table_x * 4 + table_y) * 2 + (me["c"] ^ (k & 1))
    table_token = (table_seq[:, None] * LENGTH + jnp.arange(LENGTH, dtype=jnp.int32)).reshape(-1)
    table = table.reshape(-1)

    def looked_up(tokens):
        found = jnp.where(tokens[:, None] == table_token[None, :], table[None, :], 0)
        return jnp.broadcast_to(jnp.sum(found, axis=1, keepdims=True), (tokens.shape[0], LANES))

    def candidate_of(sequence):
        same = sequence[:, None] == jnp.arange(SEQS, dtype=jnp.int32)[None, :]
        return jnp.sum(jnp.where(same, reference_order[None, :], 0), axis=1)

    sequence, position = row_place(REFERENCE, range(64), me)
    reference_at = candidate_of(sequence) * LENGTH + position
    reference_ids = looked_up(reference_at)
    sequence, position = row_place(TARGET, target_blocks, me)
    target_at = (sequence >> 1) * LENGTH + position
    target_ids = looked_up(sequence * LENGTH + position)

    def target_losses(k, start):
        return losses(
            target_passes[k],
            lax.slice_in_dim(target_ids, 512 * k, 512 * k + 512),
            own_target,
            other_target,
            start,
        )

    def reference_losses(pieces, lo, hi, start):
        return losses(
            pieces, lax.slice_in_dim(reference_ids, lo, hi), own_reference, other_reference, start
        )

    def put(stats, at, size):
        places = (at[:, None] == jnp.arange(size, dtype=jnp.int32)[None, :]).astype(jnp.bfloat16)
        return split_dot(stats, places)

    tokens = SEQS * LENGTH
    target_low = target_losses(0, bases)
    reference_low = reference_losses((r, r_first, r_second), 0, 768, after(bases, target_low))
    target_put = put(target_low, target_at[:512], tokens // 2)
    reference_put = put(reference_low, reference_at[:768], tokens)
    target_high = target_losses(1, after(bases, (target_put, reference_put)))
    target_put += put(target_high, target_at[512:], tokens // 2)
    reference_high = reference_losses((r_both,), 768, 1024, after(bases, target_put))
    reference_put += put(reference_high, reference_at[768:], tokens)
    target_put = target_put.reshape(2, 8, 1, LENGTH)
    reference_put = reference_put.reshape(2, 8, 2, LENGTH)
    payload = jnp.concatenate([target_put, reference_put], axis=2)
    payload = jnp.moveaxis(payload, 0, 1).reshape(8, 1, 6, LENGTH)
    payload = jnp.pad(payload, ((0, 0), (0, 0), (0, 2), (0, 0)))
    payload = jnp.broadcast_to(payload, (8, 8, 8, LENGTH)).reshape(64, 8, LENGTH)
    parts = lax.all_to_all(payload, CHIPS, 0, 0, tiled=True)
    peak = jnp.max(parts[:, :3], axis=0)
    whole = peak + jnp.log(jnp.sum(jnp.exp(parts[:, :3] - peak[None]), axis=0))
    loss = whole - jnp.sum(parts[:, 3:6], axis=0)

    core = me["c"]
    mine_target = loss[0]
    kept = jnp.where(core == 0, loss[1], loss[2])
    given = jnp.where(core == 0, loss[2], loss[1])
    taken = sent(given[None], sibling)[0]
    candidate = lax.axis_index(DP)
    holder = jnp.sum(jnp.where(reference_order == candidate, k & 1, 0))
    mine_reference = jnp.where(holder == core, kept, taken)
    reducible = jnp.mean(mine_target - mine_reference).reshape(1)
    return mine_target, mine_reference, reducible


def solution(mesh):
    torus = Mesh(mesh.devices.reshape(2, 4, 2, 4, 2), AXES)
    in_specs = (P(DP, MP), P(), P(None, AXES), P(AXES, None), P(), P(None, AXES), P(DP), P())
    out_specs = (P(DP), P(DP), P(DP))
    return jax.shard_map(
        shards, mesh=torus, in_specs=in_specs, out_specs=out_specs, check_vma=False
    )
```

```python
import functools

import jax
import jax.numpy as jnp
from jax import lax
from jax.experimental import pallas as pl
from jax.experimental.pallas import tpu as pltpu
from jax.sharding import Mesh
from jax.sharding import PartitionSpec as P


LENGTH = 128
SEQS = 16
EPSILON = 1e-05
LANES = 128
TILE = 256
AXES = ("xh", "y", "c", "z", "xl")
CHIPS = ("xh", "y", "z", "xl")
DP = ("xh", "y", "c")
MP = ("z", "xl")


def linear(x, y, z, c):
    return ((((x // 2) * 4 + y) * 2 + c) * 4 + z) * 2 + x % 2


def route(move):
    pairs = []
    for x in range(4):
        for y in range(4):
            for z in range(4):
                for c in range(2):
                    pairs.append((linear(x, y, z, c), linear(*move(x, y, z, c))))
    return pairs


def sent(values, move):
    return lax.ppermute(values, AXES, route(move))


def sibling(x, y, z, c):
    return x, y, z, 1 - c


def paired(axes, masks):
    def move(x, y, z, c):
        at = {"x": x, "y": y, "z": z}
        at[axes[c]] ^= masks[c]
        return at["x"], at["y"], at["z"], c

    return move


def after(values, others):
    return lax.optimization_barrier((values, others))[0]


def normalize(states, gain):
    values = states.astype(jnp.float32)
    factor = lax.rsqrt(jnp.mean(values * values, axis=1, keepdims=True) + EPSILON)
    return (values * factor * gain[None, :]).astype(jnp.bfloat16)


def here():
    return {
        "x": lax.axis_index("xh") * 2 + lax.axis_index("xl"),
        "y": lax.axis_index("y"),
        "z": lax.axis_index("z"),
        "c": lax.axis_index("c"),
    }


def chip_of_block(block, phases, me):
    at = {a: me[a] for a in "xyz"}
    for phase, steps in enumerate(phases):
        for step, (axes, masks) in enumerate(steps):
            came = (block >> (2 * phase + step)) & 1
            for core in range(2):
                moved = jnp.where(me["c"] == core, came * masks[core], 0)
                at[axes[core]] = at[axes[core]] ^ moved
    return at


def row_place(phases, blocks, me):
    k = jnp.arange(16 * len(blocks), dtype=jnp.int32)
    block = jnp.concatenate([jnp.full((16,), b, jnp.int32) for b in blocks])
    at = chip_of_block(block, phases, me)
    sequence = ((at["x"] >> 1) * 4 + at["y"]) * 2 + me["c"]
    return sequence, (at["z"] * 2 + (at["x"] & 1)) * 16 + k % 16


def gathered(pieces, start, ids_ref, refs):
    rows_ref, want_ref, top_ref, sum_ref, hit_ref = refs
    at = 0
    for piece in pieces:
        rows_ref[at : at + piece.shape[0], :] = piece[...]
        at += piece.shape[0]
    for r in range(0, at, LANES):
        k = (start + r) // LANES
        want_ref[r : r + LANES, :] = jnp.broadcast_to(ids_ref[k : k + 1, :], (LANES, LANES)).T
    top_ref[...] = jnp.full_like(top_ref, -jnp.inf)
    sum_ref[...] = jnp.zeros_like(sum_ref)
    hit_ref[...] = jnp.zeros_like(hit_ref)


def advanced(j, width, base_ref, heads, refs):
    rows_ref, want_ref, top_ref, sum_ref, hit_ref = refs
    x = rows_ref[...]
    size = heads[0].shape[0]
    lane = lax.broadcasted_iota(jnp.int32, (x.shape[0], LANES), 1)
    ids = want_ref[...]
    hit = hit_ref[...]
    top = top_ref[...]
    best = top
    groups = []
    for side, head_ref in enumerate(heads):
        logits = lax.dot_general(
            x, head_ref[...], (((1,), (1,)), ((), ())), preferred_element_type=jnp.float32
        )
        for g in range(size // LANES):
            column = lane + (j * size + g * LANES)
            part = jnp.where(column < width, logits[:, g * LANES : (g + 1) * LANES], -jnp.inf)
            wanted = jnp.where(column < width, column + base_ref[side], -1) == ids
            hit = hit + jnp.where(wanted, part, 0.0)
            best = jnp.maximum(best, part)
            groups.append(part)
    total = sum_ref[...] * jnp.exp(top - best)
    for part in groups:
        total = total + jnp.exp(part - best)
    top_ref[...] = best
    sum_ref[...] = total
    hit_ref[...] = hit


def finished(refs, out_ref):
    _, _, top_ref, sum_ref, hit_ref = refs
    for r in range(0, top_ref.shape[0], LANES):
        tops = top_ref[r : r + LANES, :].T
        sums = sum_ref[r : r + LANES, :].T
        hits = hit_ref[r : r + LANES, :].T
        peak = jnp.max(tops, axis=0, keepdims=True)
        whole = jnp.sum(sums * jnp.exp(tops - peak), axis=0, keepdims=True)
        found = jnp.concatenate(
            [peak + jnp.log(whole), jnp.sum(hits, axis=0, keepdims=True)], axis=0
        )
        high = found.astype(jnp.bfloat16).astype(jnp.float32)
        middle = (found - high).astype(jnp.bfloat16).astype(jnp.float32)
        parts = [high, middle, (found - high) - middle, jnp.zeros_like(found)]
        out_ref[:, r : r + LANES] = jnp.concatenate(parts, axis=0).astype(jnp.bfloat16)


def loss_kernel(plan, width, base_ref, *refs):
    inputs, outs, scratch = refs[: -6 * len(plan)], refs[-6 * len(plan) : -5 * len(plan)], refs[-5 * len(plan) :]
    j = pl.program_id(0)
    first = 0
    for k, (count, start, steps) in enumerate(plan):
        pieces, (ids_ref, *heads) = inputs[:count], inputs[count : count + 3]
        inputs = inputs[count + 3 :]
        mine = scratch[5 * k : 5 * k + 5]
        local = j - first

        @pl.when(local == 0)
        def _(pieces=pieces, start=start, ids_ref=ids_ref, mine=mine):
            gathered(pieces, start, ids_ref, mine)

        def body(heads=heads, mine=mine, local=local):
            advanced(local, width, base_ref, heads, mine)

        if len(plan) == 1:
            body()
        else:
            pl.when((local >= 0) & (local < steps))(body)

        @pl.when(local == steps - 1)
        def _(mine=mine, k=k):
            finished(mine, outs[k])

        first += steps


def losses(bases, *sections):
    whole = lambda shape: pl.BlockSpec(shape, lambda j: (0, 0))
    plan, in_specs, operands, out_specs, out_shape, scratch = [], [], [], [], [], []
    first = flops = moved = 0
    for pieces, start, ids, own, other in sections:
        rows = sum(p.shape[0] for p in pieces)
        width, depth = own.shape
        size = 2 * TILE if depth <= 2048 else TILE
        steps = pl.cdiv(width, size)
        tile = pl.BlockSpec(
            (size, depth),
            lambda j, first=first, steps=steps: (jnp.clip(j - first, 0, steps - 1), 0),
        )
        plan.append((len(pieces), start, steps))
        in_specs += [whole(p.shape) for p in pieces] + [whole(ids.shape), tile, tile]
        operands += [*pieces, ids, own, other]
        out_specs.append(whole((8, rows)))
        out_shape.append(jax.ShapeDtypeStruct((8, rows), jnp.bfloat16))
        scratch += [
            pltpu.VMEM((rows, depth), jnp.bfloat16),
            pltpu.VMEM((rows, LANES), jnp.int32),
            pltpu.VMEM((rows, LANES), jnp.float32),
            pltpu.VMEM((rows, LANES), jnp.float32),
            pltpu.VMEM((rows, LANES), jnp.float32),
        ]
        first += steps
        flops += 4 * rows * depth * width
        moved += 4 * depth * width + 2 * rows * depth
    return pl.pallas_call(
        functools.partial(loss_kernel, plan, width),
        grid=(first,),
        in_specs=[pl.BlockSpec(memory_space=pltpu.SMEM)] + in_specs,
        out_specs=out_specs,
        out_shape=out_shape,
        scratch_shapes=scratch,
        cost_estimate=pl.CostEstimate(flops=flops, bytes_accessed=moved, transcendentals=0),
    )(bases, *operands)


def put(parts, places):
    found = jnp.dot(jnp.concatenate(parts, axis=1), places, preferred_element_type=jnp.float32)
    return (found[0:2] + found[2:4]) + found[4:6]


def one_hot(sequence, position):
    at = (sequence >> 1) * LENGTH + position
    return (at[:, None] == jnp.arange(8 * LENGTH, dtype=jnp.int32)[None, :]).astype(jnp.bfloat16)


REFERENCE = [[((a, a), (1, 3)), ((a, a), (3, 1))] for a in "yxz"]
TARGET = [[(a, (1, 1)), (a, (3, 3))] for a in ("xz", "zy", "yx")]


TARGET_BLOCKS = [*range(24), *range(32, 40), *range(24, 32), *range(40, 64)]


def coded(ids):
    digits = jnp.stack([ids & 255, (ids >> 8) & 255, ids >> 16]).reshape(6, LANES)
    return jnp.pad(digits, ((0, 10), (0, 0))).astype(jnp.bfloat16)


def all_ids(codes, me):
    digits = codes.reshape(16, 16, LANES)[:, :6]
    digits = jnp.concatenate([digits[:4], digits[12:]]).astype(jnp.float32).astype(jnp.int32)
    digits = digits.reshape(8, 3, 2, LANES)
    table = digits[:, 0] + digits[:, 1] * 256 + digits[:, 2] * 65536
    k = jnp.arange(2 * 8, dtype=jnp.int32)
    block = (k >> 1) + jnp.where(k >= 8, 8, 0)
    at = chip_of_block(block, REFERENCE, me)
    sequence = ((at["x"] >> 1) * 4 + at["y"]) * 2 + (me["c"] ^ (k & 1))
    token = (sequence[:, None] * LENGTH + jnp.arange(LENGTH, dtype=jnp.int32)).reshape(-1)
    return token.reshape(-1, 2, LENGTH), table


def looked_up(tokens, table_token, table):
    same = tokens[:, None] == table_token.reshape(1, -1)
    found = jnp.where(same, table.reshape(1, -1), 0)
    return jnp.sum(found, axis=1).reshape(-1, LANES)


def candidate_of(reference_order, sequence):
    same = sequence[:, None] == jnp.arange(SEQS, dtype=jnp.int32)[None, :]
    return jnp.sum(jnp.where(same, reference_order[None, :], 0), axis=1)


def shards(
    target_states,
    target_gain,
    target_head,
    reference_states,
    reference_gain,
    reference_head,
    token_ids,
    reference_order,
):
    me = here()
    width = target_head.shape[1]
    my_place = lax.axis_index(AXES)
    bases = jnp.stack([my_place, my_place ^ 8]).astype(jnp.int32) * width

    own_target, own_reference = target_head.T, reference_head.T
    mine = lax.all_to_all(target_states.reshape(8, 16, 512), MP, 0, 0, tiled=True)
    ids = token_ids.reshape(1, LENGTH)
    ids = jnp.concatenate([ids, sent(ids, sibling)])
    depth = reference_states.shape[1]
    r = jnp.concatenate([normalize(reference_states, reference_gain), coded(ids)], axis=1)
    t = normalize(jnp.moveaxis(mine, 0, 1).reshape(16, 4096), target_gain)
    other_target = sent(own_target, sibling)
    other_reference = sent(own_reference, sibling)
    for k in range(2):
        t = jnp.concatenate([t, sent(t, paired(*TARGET[0][k]))])
    for k in range(4):
        came = sent(r, paired(*REFERENCE[k // 2][k % 2]))
        if k < 3:
            r = jnp.concatenate([r, came])
        if k == 2:
            names = list(me)
            *late, order_late = lax.optimization_barrier((*me.values(), reference_order, came))[:-1]
            late = dict(zip(names, late))
    codes = jnp.concatenate([r[:, depth:], came[:, depth:]])
    r = jnp.concatenate([r[:, :depth], came[:, :depth]])

    reference_at = row_place(REFERENCE, range(64), late)
    target_at = row_place(TARGET, TARGET_BLOCKS, late)
    places = one_hot(*target_at), one_hot(*reference_at)
    first, second = (paired(*step) for step in TARGET[1])
    t_first, t_second = sent(t, first), sent(t, second)
    low = jnp.concatenate([t, t_first])
    high = jnp.concatenate([t_second, sent(t_first, second)])
    first, second = (paired(*step) for step in TARGET[2])
    low_first, high_second = sent(low, first), sent(high, second)
    high_first, low_second = sent(high, first), sent(low, second)
    first, second = (paired(*step) for step in REFERENCE[2])
    r_first, r_second = sent(r, first), sent(r, second)

    token, table = all_ids(codes, late)
    candidate = candidate_of(order_late, reference_at[0])
    reference_ids = looked_up(candidate * LENGTH + reference_at[1], token, table)
    target_ids = looked_up(target_at[0] * LENGTH + target_at[1], token[:, :1], table[:, :1])
    forwarded, reference_ids, target_ids = lax.optimization_barrier(
        (low_first, reference_ids, target_ids)
    )

    low_both = sent(forwarded, paired(*TARGET[2][1]))
    high_both = sent(high_second, paired(*TARGET[2][0]))
    r_both = sent(r_first, second)
    target_passes = (
        (low, high, low_first, low_second),
        (high_first, high_second, low_both, high_both),
    )
    target = (target_ids, own_target, other_target)
    reference = (reference_ids, own_reference, other_reference)
    (target_low,) = losses(bases, (target_passes[0], 0, *target))
    (reference_low,) = losses(
        after(bases, target_low), ((r, r_first, r_second), 0, *reference)
    )
    target_high, reference_high = losses(
        after(bases, reference_low),
        (target_passes[1], 512, *target),
        ((r_both,), 768, *reference),
    )
    core = me["c"]
    target_put = put((target_low, target_high), places[0]).reshape(2, 8, 1, LENGTH)
    reference_put = put((reference_low, reference_high), places[1]).reshape(2, 1, 8, LENGTH)
    mine_order = jnp.where(core == 0, reference_order[0::2], reference_order[1::2])
    held = mine_order[None, :] == jnp.arange(SEQS, dtype=jnp.int32)[:, None]
    reference_put = jnp.sum(jnp.where(held[None, :, :, None], reference_put, 0.0), axis=2)
    reference_put = reference_put.reshape(2, 8, 2, LENGTH)
    payload = jnp.concatenate([target_put, reference_put], axis=2)
    payload = jnp.moveaxis(payload, 0, 1).reshape(8, 1, 6, LENGTH)
    payload = jnp.pad(payload, ((0, 0), (0, 0), (0, 2), (0, 0)))
    payload = jnp.broadcast_to(payload, (8, 8, 8, LENGTH)).reshape(64, 8, LENGTH)
    parts = lax.all_to_all(payload, CHIPS, 0, 0, tiled=True)
    peak = jnp.max(parts[:, :3], axis=0)
    whole = peak + jnp.log(jnp.sum(jnp.exp(parts[:, :3] - peak[None]), axis=0))
    loss = whole - jnp.sum(parts[:, 3:6], axis=0)

    mine_target = loss[0]
    kept = jnp.where(core == 0, loss[1], loss[2])
    given = jnp.where(core == 0, loss[2], loss[1])
    taken = sent(given[None], sibling)[0]
    candidate = lax.axis_index(DP)
    k = jnp.arange(SEQS, dtype=jnp.int32)
    holder = jnp.sum(jnp.where(reference_order == candidate, k & 1, 0))
    mine_reference = jnp.where(holder == core, kept, taken)
    reducible = jnp.mean(mine_target - mine_reference).reshape(1)
    return mine_target, mine_reference, reducible


def solution(mesh):
    torus = Mesh(mesh.devices.reshape(2, 4, 2, 4, 2), AXES)
    in_specs = (P(DP, MP), P(), P(None, AXES), P(AXES, None), P(), P(None, AXES), P(DP), P())
    out_specs = (P(DP), P(DP), P(DP))
    return jax.shard_map(
        shards, mesh=torus, in_specs=in_specs, out_specs=out_specs, check_vma=False
    )
```
